32 devices in a mesh: tiles: 2 (over x), slab: 16 (over z, y, core).
Axes of the slice: x: 2, y: 2, z: 4, core: 2. Of those that a mesh axis runs over, the one named last changes fastest.
Arguments:
- transmission: float32 [8192, 4096], P(('tiles', 'slab')), parts along dimension 0, may hold values from -6 to 6
- kernel_spectra: float32 [12, 2, 256, 256], replicated, may hold values from -6 to 6
Outputs:
- resist_image: float32 [8192, 256], P(('tiles', 'slab')), parts along dimension 0
The draws below stay inside these ranges and needn't reach their ends.
There are 2 independent parts, one for each index of `tiles`. The reference program is written for one: setup_inputs(seed, part) draws one part's arguments, and reference() takes and returns one part's arrays. A program takes and returns all parts, laid end to end along the dimension named above; an argument that names none is the same for every part. Nothing has to cross between parts.
All inputs are finite; a program needn't handle non-finite values.
Results may differ from the reference program's by a relative error of at most 0.0001.
Values sent between devices are 32-bit elements; how exact they have to be, the bound alone decides.
A program may use at most 128 MiB of HBM per device.

```python
import math
import jax
import jax.numpy as jnp
from jax import lax

N = 4096
B = 256
NK = 12
COLS = 256


def shard_levels(own_key, shape, shards, least, high):
    factor_of = 1.0
    for dim, shards_of in shards:
        heights = jax.random.uniform(jax.random.fold_in(jax.random.fold_in(own_key, 6), dim), (shards_of,), jnp.float32, least / len(shards), high / len(shards))
        factor_of = factor_of * jnp.repeat(jnp.exp(heights), shape[dim] // shards_of).reshape((-1,) + (1,) * (len(shape) - 1 - dim))
    return factor_of


def scatter_about(stream_key, dims, deviation, limit, split=(), kind=jnp.bfloat16):
    loudness = shard_levels(stream_key, dims, split, -0.22, 0.18) if split else 1.0
    entries = jax.random.normal(stream_key, dims, jnp.float32) * deviation * loudness
    return jnp.minimum(jnp.maximum(entries, -limit), limit).astype(kind)


def setup_inputs(seed: int = 0, part: int = 0) -> dict:
    arg_keys = jax.random.split(jax.random.key(seed), 3)
    part_splits = jax.random.split(jax.random.fold_in(arg_keys[2], part), 3)
    return {
        "transmission": scatter_about(part_splits[0], (N, N), 1.0, 6.0, ((0, 16),), jnp.float32),
        "kernel_spectra": scatter_about(arg_keys[1], (NK, 2, B, B), 1.0, 6.0, (), jnp.float32),
    }


binomial = (0.0625, 0.25, 0.375, 0.25, 0.0625)


def phase_tables(positions, tile_side, band_size):
    frequency = jnp.arange(band_size, dtype=jnp.int32) - band_size // 2
    residue = jnp.mod(positions[:, None] * frequency[None, :], tile_side)
    angles = residue.astype(jnp.float32) * (2.0 * math.pi / tile_side)
    return jnp.cos(angles), jnp.sin(angles)


def product(left, right):
    return jnp.dot(left, right, precision=lax.Precision.HIGHEST, preferred_element_type=jnp.float32)


def contract_first(left, right):
    return lax.dot_general(left, right, (((0,), (0,)), ((), ())), precision=lax.Precision.HIGHEST, preferred_element_type=jnp.float32)


def contract_last(left, right):
    return lax.dot_general(left, right, (((1,), (1,)), ((), ())), precision=lax.Precision.HIGHEST, preferred_element_type=jnp.float32)


def kernel_intensity(row_cosine, row_sine, cosine_table, sine_table, spectrum_real, spectrum_imag, kernel_spectra, norm_factor):
    half_rows = row_cosine.shape[0]

    def accumulate(running, kernel):
        prod_real = (kernel[0] * spectrum_real - kernel[1] * spectrum_imag) * norm_factor
        prod_imag = (kernel[0] * spectrum_imag + kernel[1] * spectrum_real) * norm_factor
        left_real = product(row_cosine, prod_real) - product(row_sine, prod_imag)
        left_imag = product(row_cosine, prod_imag) + product(row_sine, prod_real)
        stacked = jnp.concatenate([left_real, left_imag], 0)
        with_cosine = contract_last(stacked, cosine_table)
        with_sine = contract_last(stacked, sine_table)
        field_real = with_cosine[:half_rows] - with_sine[half_rows:]
        field_imag = with_sine[:half_rows] + with_cosine[half_rows:]
        return running + field_real * field_real + field_imag * field_imag, None

    start = jnp.zeros((half_rows, cosine_table.shape[0]), jnp.float32)
    running, unused = lax.scan(accumulate, start, kernel_spectra)
    return running / kernel_spectra.shape[0]


def reference(transmission, kernel_spectra):
    tile_side = transmission.shape[1]
    band_size = kernel_spectra.shape[2]
    cosine_table, sine_table = phase_tables(jnp.arange(tile_side, dtype=jnp.int32), tile_side, band_size)
    window_positions = jnp.mod(jnp.arange(COLS + 4, dtype=jnp.int32) - 2, tile_side).astype(jnp.int32)
    out_cosine, out_sine = phase_tables(window_positions, tile_side, band_size)
    column_real = product(transmission, cosine_table)
    column_imag = -product(transmission, sine_table)
    spectrum_real = contract_first(cosine_table, column_real) + contract_first(sine_table, column_imag)
    spectrum_imag = contract_first(cosine_table, column_imag) - contract_first(sine_table, column_real)
    norm_factor = 1.0 / (tile_side * band_size)
    intensity = kernel_intensity(cosine_table, sine_table, out_cosine, out_sine, spectrum_real, spectrum_imag, kernel_spectra, norm_factor)
    row_blurred = jnp.zeros_like(intensity)
    for position, weight in enumerate(binomial):
        row_blurred = row_blurred + weight * jnp.roll(intensity, 2 - position, axis=0)
    resist_image = jnp.zeros((tile_side, COLS), jnp.float32)
    for position, weight in enumerate(binomial):
        resist_image = resist_image + weight * row_blurred[:, position:position + COLS]
    return resist_image
```

```python
import functools
import math

import jax
import jax.numpy as jnp
import numpy as np
from jax import lax
from jax.experimental import pallas as pl
from jax.experimental.pallas import tpu as pltpu
from jax.sharding import PartitionSpec as P

COLS = 256
LANES = 128
CHUNK = 512
binomial = (0.0625, 0.25, 0.375, 0.25, 0.0625)
MESH = pl.DeviceIdType.MESH


def halves_of(table):
    high = np.asarray(table, np.float32).astype(jnp.bfloat16)
    low = (np.asarray(table, np.float64) - high.astype(np.float64)).astype(jnp.bfloat16)
    return high, low


def angle(positions, frequency, side):
    residue = np.mod(np.outer(positions, frequency), side)
    return residue.astype(np.float64) * (2.0 * math.pi / side)


@functools.lru_cache(maxsize=None)
def tables(slabs, rows, side, band, chunk):
    frequency = np.arange(band) - band // 2
    even, odd = frequency[0::2], frequency[1::2]
    y = np.arange(chunk)
    column = np.concatenate(
        [f(angle(y, g, side)) for g in (even, odd) for f in (np.cos, np.sin)], axis=1
    )
    both = np.concatenate([even, odd])
    starts = np.arange(side // 2 // chunk) * chunk
    turn = angle(starts, both, side)
    twiddle = np.stack([np.cos(turn), np.sin(turn)], axis=1).astype(np.float32)
    order = (both[:, None] == frequency[None, :]).astype(jnp.bfloat16)
    x = angle(np.arange(rows), frequency, side).T
    row = np.concatenate([np.cos(x), np.sin(x)], axis=0)
    lanes = -(-slabs // LANES) * LANES
    first = angle(np.arange(lanes) * rows, frequency, side).T
    phase = np.stack([np.cos(first), np.sin(first)]).astype(np.float32)
    total = 2 * band
    stride = side // total
    s = angle(np.arange(0, rows, stride), frequency, side)
    c, d = np.cos(s), np.sin(s)
    sample = np.concatenate(
        [np.concatenate([c, -d], 1), np.concatenate([d, c], 1)], axis=0
    )
    wide = -(-(COLS + 4) // LANES) * LANES
    q = angle(np.arange(wide) - 2, frequency, side).T
    window = np.concatenate([np.cos(q), np.sin(q)], axis=1)
    g = np.arange(-(band - 1), band)
    gain = sum(w * np.cos(angle([u - 2], g, side))[0] for u, w in enumerate(binomial)) / total
    shift = np.arange(side)
    kernel = np.cos(angle(shift, g, side)) @ gain
    index = np.mod(np.arange(rows)[:, None] - stride * np.arange(total)[None, :], side)
    spread = kernel[index]
    return dict(
        column=np.stack(halves_of(column)),
        twiddle=twiddle,
        order=order,
        row=np.stack(halves_of(row)),
        phase=phase,
        sample=np.concatenate(halves_of(sample), axis=0),
        window=np.stack(halves_of(window)),
        spread=np.stack(halves_of(spread)),
    )


NAMES = ("column", "twiddle", "order", "row", "phase", "sample", "window", "spread")


def split(x):
    high = x.astype(jnp.bfloat16)
    return high, (x - high.astype(jnp.float32)).astype(jnp.bfloat16)


def dot(a, b):
    return jnp.dot(a, b, preferred_element_type=jnp.float32)


def dot3(a, b):
    return dot(a[0], b[0]) + dot(a[0], b[1]) + dot(a[1], b[0])


def body(slabs, chunk, t_hbm, k_hbm, *refs):
    count = len(NAMES)
    hbm = dict(zip(NAMES, refs[:count]))
    out = refs[count]
    scratch = refs[count + 1 :]
    t_ref, k_ref = scratch[:2]
    tab = dict(zip(NAMES, scratch[2 : 2 + count]))
    (acc, sbuf, rbuf, fbuf, spec, lbuf, ibuf, load_sem, t_sem, ssem, rsem) = scratch[2 + count :]
    me = lax.axis_index("slab")
    rows, side = t_ref.shape
    kernels, _, band, _ = k_ref.shape
    half = side // 2
    steps = half // chunk
    part = sbuf.shape[0] // slabs
    samples = ibuf.shape[1]

    def peer(k):
        return lax.rem(me + k, slabs)

    barrier = pltpu.get_barrier_semaphore()
    for k in range(1, slabs):
        pl.semaphore_signal(barrier, inc=1, device_id={"slab": peer(k)}, device_id_type=MESH)

    loads = {}
    for i, name in enumerate(NAMES):
        loads[name] = pltpu.make_async_copy(hbm[name], tab[name], load_sem.at[i])
    t_loads = []
    for c in range(steps):
        for h in range(2):
            lanes = pl.ds(h * half + c * chunk, chunk)
            t_loads.append(
                pltpu.make_async_copy(
                    t_hbm.at[:, lanes], t_ref.at[:, lanes], t_sem.at[2 * c + h]
                )
            )
    k_load = pltpu.make_async_copy(k_hbm, k_ref, load_sem.at[count])
    t_loads[0].start()
    t_loads[1].start()
    loads["column"].start()
    loads["twiddle"].start()
    for load in t_loads[2:]:
        load.start()
    for name in ("order", "row", "phase"):
        loads[name].start()
    k_load.start()
    for name in ("sample", "window", "spread"):
        loads[name].start()

    for c in range(steps):
        t_loads[2 * c].wait()
        t_loads[2 * c + 1].wait()
        if c == 0:
            loads["column"].wait()
            loads["twiddle"].wait()
        left = t_ref[:, c * chunk : (c + 1) * chunk]
        right = t_ref[:, half + c * chunk : half + (c + 1) * chunk]
        for j, folded in enumerate((left + right, left - right)):
            lanes = slice(j * band, (j + 1) * band)
            table = (tab["column"][0, :, lanes], tab["column"][1, :, lanes])
            got = dot3(split(folded), table)
            cosine, sine = got[:, : band // 2], got[:, band // 2 :]
            near = slice(j * band // 2, (j + 1) * band // 2)
            far = slice(band + j * band // 2, band + (j + 1) * band // 2)
            if c == 0:
                acc[:, near] = cosine
                acc[:, far] = sine
            else:
                tc = tab["twiddle"][c, 0:1, near]
                ts = tab["twiddle"][c, 1:2, near]
                acc[:, near] += cosine * tc - sine * ts
                acc[:, far] += sine * tc + cosine * ts

    loads["order"].wait()
    loads["row"].wait()
    loads["phase"].wait()
    ordered = []
    for lanes in (slice(0, band), slice(band, 2 * band)):
        ordered.append([dot(p, tab["order"][...]).astype(jnp.bfloat16) for p in split(acc[:, lanes])])
    columns = [jnp.concatenate([ordered[0][i], ordered[1][i]], axis=1) for i in range(2)]
    z = dot3((tab["row"][0], tab["row"][1]), columns)
    re = z[:band, :band] - z[band:, band:]
    im = -(z[:band, band:] + z[band:, :band])
    lane = lax.broadcasted_iota(jnp.int32, tab["phase"].shape[1:], 1)
    pc = jnp.sum(jnp.where(lane == me, tab["phase"][0], 0.0), axis=1, keepdims=True)
    ps = jnp.sum(jnp.where(lane == me, tab["phase"][1], 0.0), axis=1, keepdims=True)
    sbuf[:band, :] = re * pc + im * ps
    sbuf[band:, :] = im * pc - re * ps

    pl.semaphore_wait(barrier, slabs - 1)
    sends = []
    for k in range(1, slabs):
        to = peer(k)
        sends.append(
            pltpu.make_async_remote_copy(
                src_ref=sbuf.at[pl.ds(pl.multiple_of(to * part, part), part)],
                dst_ref=rbuf.at[k - 1],
                send_sem=ssem.at[0, k - 1],
                recv_sem=rsem.at[0, k - 1],
                device_id={"slab": to},
                device_id_type=MESH,
            )
        )
        sends[-1].start()
    own = pl.ds(pl.multiple_of(me * part, part), part)
    total = sbuf[own, :]
    for k in range(1, slabs):
        sends[k - 1].wait_recv()
        total = total + rbuf[k - 1]
    fbuf[own, :] = total
    shares = []
    for k in range(1, slabs):
        shares.append(
            pltpu.make_async_remote_copy(
                src_ref=fbuf.at[own],
                dst_ref=fbuf.at[own],
                send_sem=ssem.at[1, k - 1],
                recv_sem=rsem.at[1, k - 1],
                device_id={"slab": peer(k)},
                device_id_type=MESH,
            )
        )
        shares[-1].start()
    for send in sends:
        send.wait_send()
    k_load.wait()
    for name in ("sample", "window", "spread"):
        loads[name].wait()
    for share in shares:
        share.wait_recv()

    norm = 1.0 / (side * band)
    re, im = fbuf[:band, :], fbuf[band:, :]
    spec[:band, :] = (re * pc - im * ps) * norm
    spec[band:, :] = (im * pc + re * ps) * norm

    def one(k, carry):
        sr, si = spec[:band, :], spec[band:, :]
        kr, ki = k_ref[k, 0], k_ref[k, 1]
        rh, rl = split(kr * sr - ki * si)
        ih, il = split(kr * si + ki * sr)
        high = jnp.concatenate([rh, ih], axis=0)
        low = jnp.concatenate([rl, il], axis=0)
        wide = dot(tab["sample"][...], high)
        lbuf[k] = wide[: 2 * samples] + wide[2 * samples :] + dot(tab["sample"][: 2 * samples, :], low)
        return carry

    lax.fori_loop(0, kernels, one, 0)
    left = split(lbuf[...].reshape(kernels * 2 * samples, band))
    field = dot3(left, (tab["window"][0], tab["window"][1]))
    width = field.shape[1] // 2
    field = field.reshape(kernels, 2 * samples, 2 * width)
    fr = field[:, :samples, :width] - field[:, samples:, width:]
    fi = field[:, :samples, width:] + field[:, samples:, :width]
    intensity = jnp.sum(fr * fr + fi * fi, axis=0) * (1.0 / kernels)
    blurred = binomial[0] * intensity
    for v in range(1, 5):
        blurred = blurred + binomial[v] * pltpu.roll(intensity, width - v, 1)
    ibuf[0] = blurred[:, :COLS]

    rings = []
    for k in range(1, slabs):
        rings.append(
            pltpu.make_async_remote_copy(
                src_ref=ibuf.at[0],
                dst_ref=ibuf.at[slabs - k],
                send_sem=ssem.at[2, k - 1],
                recv_sem=rsem.at[2, k - 1],
                device_id={"slab": peer(k)},
                device_id_type=MESH,
            )
        )
        rings[-1].start()
    for share in shares:
        share.wait_send()
    for ring in rings:
        ring.wait_recv()
    gathered = split(ibuf[...].reshape(slabs * samples, COLS))
    out[...] = dot3((tab["spread"][0], tab["spread"][1]), gathered)
    for ring in rings:
        ring.wait_send()


def local(transmission, kernel_spectra):
    slabs = lax.axis_size("slab")
    rows, side = transmission.shape
    kernels, _, band, _ = kernel_spectra.shape
    chunk = min(CHUNK, side // 2)
    consts = tables(slabs, rows, side, band, chunk)
    arrays = [jnp.asarray(consts[name]) for name in NAMES]
    samples = rows * 2 * band // side
    part = 2 * band // slabs
    any_spec = pl.BlockSpec(memory_space=pl.ANY)
    return pl.pallas_call(
        functools.partial(body, slabs, chunk),
        out_shape=jax.ShapeDtypeStruct((rows, COLS), jnp.float32),
        in_specs=[any_spec] * (2 + len(NAMES)),
        out_specs=pl.BlockSpec(memory_space=pltpu.VMEM),
        scratch_shapes=[
            pltpu.VMEM(transmission.shape, jnp.float32),
            pltpu.VMEM(kernel_spectra.shape, jnp.float32),
            *[pltpu.VMEM(a.shape, a.dtype) for a in arrays],
            pltpu.VMEM((rows, 2 * band), jnp.float32),
            pltpu.VMEM((2 * band, band), jnp.float32),
            pltpu.VMEM((slabs - 1, part, band), jnp.float32),
            pltpu.VMEM((2 * band, band), jnp.float32),
            pltpu.VMEM((2 * band, band), jnp.float32),
            pltpu.VMEM((kernels, 2 * samples, band), jnp.float32),
            pltpu.VMEM((slabs, samples, COLS), jnp.float32),
            pltpu.SemaphoreType.DMA((len(NAMES) + 1,)),
            pltpu.SemaphoreType.DMA((2 * (side // 2 // chunk),)),
            pltpu.SemaphoreType.DMA((3, slabs - 1)),
            pltpu.SemaphoreType.DMA((3, slabs - 1)),
        ],
        compiler_params=pltpu.CompilerParams(
            collective_id=0, has_side_effects=True, vmem_limit_bytes=48 * 1024 * 1024
        ),
    )(transmission, kernel_spectra, *arrays)


def solution(mesh):
    return jax.shard_map(
        local,
        mesh=mesh,
        in_specs=(P(("tiles", "slab"), None), P()),
        out_specs=P(("tiles", "slab"), None),
        check_vma=False,
    )
```

```python
import functools
import math

import jax
import jax.numpy as jnp
import numpy as np
from jax import lax
from jax.experimental import pallas as pl
from jax.experimental.pallas import tpu as pltpu
from jax.sharding import PartitionSpec as P

COLS = 256
LANES = 128
CHUNK = 512
binomial = (0.0625, 0.25, 0.375, 0.25, 0.0625)
MESH = pl.DeviceIdType.MESH


def halves_of(table):
    high = np.asarray(table, np.float32).astype(jnp.bfloat16)
    low = (np.asarray(table, np.float64) - high.astype(np.float64)).astype(jnp.bfloat16)
    return high, low


def angle(positions, frequency, side):
    residue = np.mod(np.outer(positions, frequency), side)
    return residue.astype(np.float64) * (2.0 * math.pi / side)


@functools.lru_cache(maxsize=None)
def tables(slabs, rows, side, band, chunk):
    frequency = np.arange(band) - band // 2
    even, odd = frequency[0::2], frequency[1::2]
    y = np.arange(chunk)
    column = np.concatenate(
        [f(angle(y, g, side)) for g in (even, odd) for f in (np.cos, np.sin)], axis=1
    )
    both = np.concatenate([even, odd])
    starts = np.arange(side // 2 // chunk) * chunk
    turn = angle(starts, both, side)
    twiddle = np.stack([np.cos(turn), np.sin(turn)], axis=1).astype(np.float32)
    order = (both[:, None] == frequency[None, :]).astype(jnp.bfloat16)
    x = angle(np.arange(rows), frequency[: band // 2], side).T
    row = np.concatenate([np.cos(x), np.sin(x)], axis=0)
    lanes = -(-slabs // LANES) * LANES
    first = angle(np.arange(lanes) * rows, frequency, side).T
    phase = np.stack([np.cos(first), np.sin(first)]).astype(np.float32)
    total = 2 * band
    stride = side // total
    s = angle(np.arange(0, rows, stride), frequency, side)
    c, d = np.cos(s), np.sin(s)
    sample = np.concatenate(
        [np.concatenate([c, -d], 1), np.concatenate([d, c], 1)], axis=0
    )
    wide = -(-(COLS + 4) // LANES) * LANES
    q = angle(np.arange(wide) - 2, frequency, side).T
    window = np.concatenate([np.cos(q), np.sin(q)], axis=1)
    g = np.arange(-(band - 1), band)
    gain = sum(w * np.cos(angle([u - 2], g, side))[0] for u, w in enumerate(binomial)) / total
    shift = np.arange(side)
    kernel = np.cos(angle(shift, g, side)) @ gain
    index = np.mod(np.arange(rows)[:, None] - stride * np.arange(total)[None, :], side)
    spread = kernel[index]
    return dict(
        column=np.stack(halves_of(column)),
        twiddle=twiddle,
        order=order,
        row=np.stack(halves_of(row)),
        phase=phase,
        sample=np.concatenate(halves_of(sample), axis=0),
        window=np.stack(halves_of(window)),
        spread=np.stack(halves_of(spread)),
    )


NAMES = ("column", "twiddle", "order", "row", "phase", "sample", "window", "spread")


def split(x):
    high = x.astype(jnp.bfloat16)
    return high, (x - high.astype(jnp.float32)).astype(jnp.bfloat16)


def dot(a, b):
    return jnp.dot(a, b, preferred_element_type=jnp.float32)


def dot3(a, b):
    return dot(a[0], b[0]) + dot(a[0], b[1]) + dot(a[1], b[0])


def body(slabs, chunk, t_hbm, k_hbm, *refs):
    count = len(NAMES)
    hbm = dict(zip(NAMES, refs[:count]))
    out = refs[count]
    scratch = refs[count + 1 :]
    t_ref, k_ref = scratch[:2]
    tab = dict(zip(NAMES, scratch[2 : 2 + count]))
    (acc, sbuf, pbuf, csum, rbuf, fbuf, esend, epsum, erecv, spec, lbuf, ibuf, load_sem, t_sem, ssem, rsem) = scratch[2 + count :]
    me = lax.axis_index("slab")
    rows, side = t_ref.shape
    kernels, _, band, _ = k_ref.shape
    half = side // 2
    steps = half // chunk
    part = sbuf.shape[0] // slabs
    samples = ibuf.shape[1]

    chips = slabs // 2
    chip, core = me // 2, lax.rem(me, 2)
    partner = me + 1 - 2 * core
    low = band // 2

    def peer(k):
        return 2 * lax.rem(chip + k, chips) + core

    def place(of_chip, of_core):
        return pl.ds(pl.multiple_of((of_core * chips + of_chip) * part, part), part)

    def remote(src, dst, phase, index, to):
        return pltpu.make_async_remote_copy(
            src_ref=src,
            dst_ref=dst,
            send_sem=ssem.at[phase, index],
            recv_sem=rsem.at[phase, index],
            device_id={"slab": to},
            device_id_type=MESH,
        )

    barrier = pltpu.get_barrier_semaphore()
    for to in [partner] + [peer(k) for k in range(1, chips)]:
        pl.semaphore_signal(barrier, inc=1, device_id={"slab": to}, device_id_type=MESH)

    loads = {}
    for i, name in enumerate(NAMES):
        loads[name] = pltpu.make_async_copy(hbm[name], tab[name], load_sem.at[i])
    t_loads = []
    for c in range(steps):
        for h in range(2):
            lanes = pl.ds(h * half + c * chunk, chunk)
            t_loads.append(
                pltpu.make_async_copy(
                    t_hbm.at[:, lanes], t_ref.at[:, lanes], t_sem.at[2 * c + h]
                )
            )
    k_load = pltpu.make_async_copy(k_hbm, k_ref, load_sem.at[count])
    t_loads[0].start()
    t_loads[1].start()
    loads["column"].start()
    loads["twiddle"].start()
    for load in t_loads[2:]:
        load.start()
    for name in ("order", "row", "phase"):
        loads[name].start()
    k_load.start()
    for name in ("sample", "window", "spread"):
        loads[name].start()

    for c in range(steps):
        t_loads[2 * c].wait()
        t_loads[2 * c + 1].wait()
        if c == 0:
            loads["column"].wait()
            loads["twiddle"].wait()
        left = t_ref[:, c * chunk : (c + 1) * chunk]
        right = t_ref[:, half + c * chunk : half + (c + 1) * chunk]
        for j, folded in enumerate((left + right, left - right)):
            lanes = slice(j * band, (j + 1) * band)
            table = (tab["column"][0, :, lanes], tab["column"][1, :, lanes])
            got = dot3(split(folded), table)
            cosine, sine = got[:, : band // 2], got[:, band // 2 :]
            near = slice(j * band // 2, (j + 1) * band // 2)
            far = slice(band + j * band // 2, band + (j + 1) * band // 2)
            if c == 0:
                acc[:, near] = cosine
                acc[:, far] = sine
            else:
                tc = tab["twiddle"][c, 0:1, near]
                ts = tab["twiddle"][c, 1:2, near]
                acc[:, near] += cosine * tc - sine * ts
                acc[:, far] += sine * tc + cosine * ts

    loads["order"].wait()
    loads["row"].wait()
    loads["phase"].wait()
    ordered = [
        [dot(p, tab["order"][...]) for p in split(acc[:, lanes])]
        for lanes in (slice(0, band), slice(band, 2 * band))
    ]
    columns = [
        jnp.concatenate([ordered[0][i].astype(jnp.bfloat16), ordered[1][i].astype(jnp.bfloat16)], axis=1)
        for i in range(2)
    ]
    z = dot3((tab["row"][0], tab["row"][1]), columns)
    zcc, zcs, zsc, zss = z[:low, :band], z[:low, band:], z[low:, :band], z[low:, band:]
    lane = lax.broadcasted_iota(jnp.int32, tab["phase"].shape[1:], 1)
    pc = jnp.sum(jnp.where(lane == me, tab["phase"][0], 0.0), axis=1, keepdims=True)
    ps = jnp.sum(jnp.where(lane == me, tab["phase"][1], 0.0), axis=1, keepdims=True)
    nc, ns = pc[:low], ps[:low]
    re, im = zcc - zss, -(zcs + zsc)
    re, im = re * nc + im * ns, im * nc - re * ns
    sbuf[:low, :] = re[:, :low]
    sbuf[low : 2 * low, :] = re[:, low:]
    sbuf[2 * low : 3 * low, :] = im[:, :low]
    sbuf[3 * low :, :] = im[:, low:]
    esend[0:1, :band] = jnp.sum(ordered[0][0] + ordered[0][1], axis=0, keepdims=True)
    esend[0:1, band : 2 * band] = -jnp.sum(ordered[1][0] + ordered[1][1], axis=0, keepdims=True)
    re, im = (zcc + zss)[:, :low], (zcs - zsc)[:, :low]
    re, im = re * nc + im * ns, im * nc - re * ns
    esend[0:1, 2 * band : 2 * band + low] = re.T[0:1]
    esend[0:1, 2 * band + low :] = im.T[0:1]

    pl.semaphore_wait(barrier, chips)
    length = chips * part
    mine = pl.ds(pl.multiple_of(core * length, length), length)
    theirs = pl.ds(pl.multiple_of((1 - core) * length, length), length)
    pair = remote(sbuf.at[theirs], pbuf, 0, 0, partner)
    epair = remote(esend, erecv.at[0], 1, 0, partner)
    pair.start()
    epair.start()
    pair.wait_recv()
    csum[...] = sbuf[mine, :] + pbuf[...]
    epair.wait_recv()
    epsum[...] = esend[...] + erecv[0]
    sends, esends = [], []
    for k in range(1, chips):
        to = lax.rem(chip + k, chips)
        piece = pl.ds(pl.multiple_of(to * part, part), part)
        sends.append(remote(csum.at[piece], rbuf.at[k - 1], 0, k, peer(k)))
        esends.append(remote(epsum, erecv.at[k], 1, k, peer(k)))
        sends[-1].start()
        esends[-1].start()
    total = csum[pl.ds(pl.multiple_of(chip * part, part), part), :]
    for k in range(1, chips):
        sends[k - 1].wait_recv()
        total = total + rbuf[k - 1]
    own = place(chip, core)
    fbuf[own, :] = total
    shares = [remote(fbuf.at[own], fbuf.at[own], 2, k, peer(k)) for k in range(1, chips)]
    for share in shares:
        share.start()
    passed = [remote(fbuf.at[own], fbuf.at[own], 3, 0, partner)]
    passed[0].start()
    edge = epsum[...]
    for k in range(1, chips):
        esends[k - 1].wait_recv()
        edge = edge + erecv[k]
    k_load.wait()
    for name in ("sample", "window", "spread"):
        loads[name].wait()
    for k in range(1, chips):
        shares[k - 1].wait_recv()
        region = fbuf.at[place(lax.rem(chip - k + chips, chips), core)]
        passed.append(remote(region, region, 3, k, partner))
        passed[-1].start()
    for p in passed:
        p.wait_recv()

    mre = jnp.concatenate([fbuf[:low, :], fbuf[low : 2 * low, :]], axis=1)
    mim = jnp.concatenate([fbuf[2 * low : 3 * low, :], fbuf[3 * low :, :]], axis=1)
    cells = [lax.broadcasted_iota(jnp.int32, (band, band), i) for i in range(2)]
    mirror = (cells[0] + cells[1] == band).astype(jnp.float32).astype(jnp.bfloat16)
    cells = [lax.broadcasted_iota(jnp.int32, (low, low), i) for i in range(2)]
    flip = (cells[0] + cells[1] == low).astype(jnp.float32).astype(jnp.bfloat16)
    turned = dot(jnp.concatenate([*split(mre), *split(mim)], axis=0), mirror)
    first = lax.broadcasted_iota(jnp.int32, (low, band), 1) == 0
    parts = []
    for i in range(2):
        both = turned[2 * i * low : (2 * i + 1) * low] + turned[(2 * i + 1) * low : (2 * i + 2) * low]
        corner = edge[:, 2 * band + i * low : 2 * band + (i + 1) * low]
        corner = jnp.broadcast_to(corner, (low, low)).T[:, 0:1]
        parts += split(jnp.where(first, corner, both))
    flipped = dot(flip, jnp.concatenate(parts, axis=1))
    top = lax.broadcasted_iota(jnp.int32, (low, band), 0) == 0
    fre = jnp.where(top, edge[:, :band], flipped[:, :band] + flipped[:, band : 2 * band])
    fim = jnp.where(top, edge[:, band : 2 * band], -(flipped[:, 2 * band : 3 * band] + flipped[:, 3 * band :]))

    norm = 1.0 / (side * band)
    re = jnp.concatenate([mre, fre], axis=0)
    im = jnp.concatenate([mim, fim], axis=0)
    spec[:band, :] = (re * pc - im * ps) * norm
    spec[band:, :] = (im * pc + re * ps) * norm

    def one(k, carry):
        sr, si = spec[:band, :], spec[band:, :]
        kr, ki = k_ref[k, 0], k_ref[k, 1]
        rh, rl = split(kr * sr - ki * si)
        ih, il = split(kr * si + ki * sr)
        high = jnp.concatenate([rh, ih], axis=0)
        low = jnp.concatenate([rl, il], axis=0)
        wide = dot(tab["sample"][...], high)
        lbuf[k] = wide[: 2 * samples] + wide[2 * samples :] + dot(tab["sample"][: 2 * samples, :], low)
        return carry

    lax.fori_loop(0, kernels, one, 0)
    left = split(lbuf[...].reshape(kernels * 2 * samples, band))
    field = dot3(left, (tab["window"][0], tab["window"][1]))
    width = field.shape[1] // 2
    field = field.reshape(kernels, 2 * samples, 2 * width)
    fr = field[:, :samples, :width] - field[:, samples:, width:]
    fi = field[:, :samples, width:] + field[:, samples:, :width]
    intensity = jnp.sum(fr * fr + fi * fi, axis=0) * (1.0 / kernels)
    blurred = binomial[0] * intensity
    for v in range(1, 5):
        blurred = blurred + binomial[v] * pltpu.roll(intensity, width - v, 1)
    ibuf[0] = blurred[:, :COLS]

    rings = [
        remote(ibuf.at[0], ibuf.at[slabs - 2 * k], 4, k, peer(k)) for k in range(1, chips)
    ]
    for ring in rings:
        ring.start()
    beside = [remote(ibuf.at[0], ibuf.at[lax.rem(slabs - 1 + 2 * core, slabs)], 5, 0, partner)]
    beside[0].start()
    for k in range(1, chips):
        rings[k - 1].wait_recv()
        slot = lax.rem(slabs - 2 * k - 1 + 2 * core + slabs, slabs)
        beside.append(remote(ibuf.at[slabs - 2 * k], ibuf.at[slot], 5, k, partner))
        beside[-1].start()
    for b in beside:
        b.wait_recv()
    gathered = split(ibuf[...].reshape(slabs * samples, COLS))
    out[...] = dot3((tab["spread"][0], tab["spread"][1]), gathered)
    for copy in [pair, epair] + sends + esends + shares + passed + rings + beside:
        copy.wait_send()


def local(transmission, kernel_spectra):
    slabs = lax.axis_size("slab")
    rows, side = transmission.shape
    kernels, _, band, _ = kernel_spectra.shape
    chunk = min(CHUNK, side // 2)
    consts = tables(slabs, rows, side, band, chunk)
    arrays = [jnp.asarray(consts[name]) for name in NAMES]
    samples = rows * 2 * band // side
    part = 2 * band // slabs
    chips, low = slabs // 2, band // 2
    any_spec = pl.BlockSpec(memory_space=pl.ANY)
    return pl.pallas_call(
        functools.partial(body, slabs, chunk),
        out_shape=jax.ShapeDtypeStruct((rows, COLS), jnp.float32),
        in_specs=[any_spec] * (2 + len(NAMES)),
        out_specs=pl.BlockSpec(memory_space=pltpu.VMEM),
        scratch_shapes=[
            pltpu.VMEM(transmission.shape, jnp.float32),
            pltpu.VMEM(kernel_spectra.shape, jnp.float32),
            *[pltpu.VMEM(a.shape, a.dtype) for a in arrays],
            pltpu.VMEM((rows, 2 * band), jnp.float32),
            pltpu.VMEM((2 * band, low), jnp.float32),
            pltpu.VMEM((chips * part, low), jnp.float32),
            pltpu.VMEM((chips * part, low), jnp.float32),
            pltpu.VMEM((chips - 1, part, low), jnp.float32),
            pltpu.VMEM((2 * band, low), jnp.float32),
            pltpu.VMEM((1, 3 * band), jnp.float32),
            pltpu.VMEM((1, 3 * band), jnp.float32),
            pltpu.VMEM((chips, 1, 3 * band), jnp.float32),
            pltpu.VMEM((2 * band, band), jnp.float32),
            pltpu.VMEM((kernels, 2 * samples, band), jnp.float32),
            pltpu.VMEM((slabs, samples, COLS), jnp.float32),
            pltpu.SemaphoreType.DMA((len(NAMES) + 1,)),
            pltpu.SemaphoreType.DMA((2 * (side // 2 // chunk),)),
            pltpu.SemaphoreType.DMA((6, chips)),
            pltpu.SemaphoreType.DMA((6, chips)),
        ],
        compiler_params=pltpu.CompilerParams(
            collective_id=0, has_side_effects=True, vmem_limit_bytes=67_043_328
        ),
    )(transmission, kernel_spectra, *arrays)


def solution(mesh):
    return jax.shard_map(
        local,
        mesh=mesh,
        in_specs=(P(("tiles", "slab"), None), P()),
        out_specs=P(("tiles", "slab"), None),
        check_vma=False,
    )
```

```python
import functools
import math

import jax
import jax.numpy as jnp
import numpy as np
from jax import lax
from jax.experimental import pallas as pl
from jax.experimental.pallas import tpu as pltpu
from jax.sharding import PartitionSpec as P

COLS = 256
LANES = 128
CHUNK = 512
binomial = (0.0625, 0.25, 0.375, 0.25, 0.0625)
MESH = pl.DeviceIdType.MESH


def halves_of(table):
    high = np.asarray(table, np.float32).astype(jnp.bfloat16)
    low = (np.asarray(table, np.float64) - high.astype(np.float64)).astype(jnp.bfloat16)
    return high, low


def angle(positions, frequency, side):
    residue = np.mod(np.outer(positions, frequency), side)
    return residue.astype(np.float64) * (2.0 * math.pi / side)


@functools.lru_cache(maxsize=None)
def tables(slabs, rows, side, band, chunk):
    frequency = np.arange(band) - band // 2
    even, odd = frequency[0::2], frequency[1::2]
    y = np.arange(chunk)
    column = np.concatenate(
        [f(angle(y, g, side)) for g in (even, odd) for f in (np.cos, np.sin)], axis=1
    )
    both = np.concatenate([even, odd])
    starts = np.arange(side // 2 // chunk) * chunk
    turn = angle(starts, both, side)
    twiddle = np.stack([np.cos(turn), np.sin(turn)], axis=1).astype(np.float32)
    order = (both[:, None] == frequency[None, :]).astype(jnp.bfloat16)
    x = angle(np.arange(rows), frequency[: band // 2], side).T
    row = np.concatenate([np.cos(x), np.sin(x)], axis=0)
    lanes = -(-slabs // LANES) * LANES
    first = angle(np.arange(lanes) * rows, frequency, side).T
    phase = np.stack([np.cos(first), np.sin(first)]).astype(np.float32)
    total = 2 * band
    stride = side // total
    s = angle(np.arange(0, rows, stride), frequency, side)
    c, d = np.cos(s), np.sin(s)
    sample = np.concatenate(
        [np.concatenate([c, -d], 1), np.concatenate([d, c], 1)], axis=0
    )
    wide = -(-(COLS + 4) // LANES) * LANES
    q = angle(np.arange(wide) - 2, frequency, side).T
    window = np.concatenate([np.cos(q), np.sin(q)], axis=1)
    g = np.arange(-(band - 1), band)
    gain = sum(w * np.cos(angle([u - 2], g, side))[0] for u, w in enumerate(binomial)) / total
    shift = np.arange(side)
    kernel = np.cos(angle(shift, g, side)) @ gain
    index = np.mod(np.arange(rows)[:, None] - stride * np.arange(total)[None, :], side)
    spread = kernel[index]
    return dict(
        column=np.stack(halves_of(column)),
        twiddle=twiddle,
        order=order,
        row=np.stack(halves_of(row)),
        phase=phase,
        sample=np.concatenate(halves_of(sample), axis=0),
        window=np.stack(halves_of(window)),
        spread=np.stack(halves_of(spread)),
    )


NAMES = ("column", "twiddle", "order", "row", "phase", "sample", "window", "spread")


def split(x):
    high = x.astype(jnp.bfloat16)
    return high, (x - high.astype(jnp.float32)).astype(jnp.bfloat16)


def dot(a, b):
    return jnp.dot(a, b, preferred_element_type=jnp.float32)


def dot3(a, b):
    return dot(a[0], b[0]) + dot(a[0], b[1]) + dot(a[1], b[0])


def body(slabs, chunk, t_hbm, k_hbm, *refs):
    count = len(NAMES)
    hbm = dict(zip(NAMES, refs[:count]))
    out = refs[count]
    scratch = refs[count + 1 :]
    t_ref, k_ref = scratch[:2]
    tab = dict(zip(NAMES, scratch[2 : 2 + count]))
    (acc, sbuf, pbuf, csum, rbuf, fbuf, esend, epsum, erecv, spec, lbuf, ibuf, load_sem, t_sem, ssem, rsem) = scratch[2 + count :]
    me = lax.axis_index("slab")
    rows, side = t_ref.shape
    kernels, _, band, _ = k_ref.shape
    half = side // 2
    steps = half // chunk
    part = sbuf.shape[0] // slabs
    samples = ibuf.shape[1]

    chips = slabs // 2
    chip, core = me // 2, lax.rem(me, 2)
    partner = me + 1 - 2 * core
    low = band // 2

    def peer(k):
        return 2 * lax.rem(chip + k, chips) + core

    def place(of_chip, of_core):
        return pl.ds(pl.multiple_of((of_core * chips + of_chip) * part, part), part)

    def remote(src, dst, phase, index, to):
        return pltpu.make_async_remote_copy(
            src_ref=src,
            dst_ref=dst,
            send_sem=ssem.at[phase, index],
            recv_sem=rsem.at[phase, index],
            device_id={"slab": to},
            device_id_type=MESH,
        )

    barrier = pltpu.get_barrier_semaphore()
    for to in [partner] + [peer(k) for k in range(1, chips)]:
        pl.semaphore_signal(barrier, inc=1, device_id={"slab": to}, device_id_type=MESH)

    loads = {}
    for i, name in enumerate(NAMES):
        loads[name] = pltpu.make_async_copy(hbm[name], tab[name], load_sem.at[i])
    t_loads = []
    for c in range(steps):
        for h in range(2):
            lanes = pl.ds(h * half + c * chunk, chunk)
            t_loads.append(
                pltpu.make_async_copy(
                    t_hbm.at[:, lanes], t_ref.at[:, lanes], t_sem.at[2 * c + h]
                )
            )
    k_load = pltpu.make_async_copy(k_hbm, k_ref, load_sem.at[count])
    t_loads[0].start()
    t_loads[1].start()
    loads["column"].start()
    loads["twiddle"].start()
    for load in t_loads[2:]:
        load.start()
    for name in ("order", "row", "phase"):
        loads[name].start()

    for c in range(steps):
        t_loads[2 * c].wait()
        t_loads[2 * c + 1].wait()
        if c == 0:
            loads["column"].wait()
            loads["twiddle"].wait()
        left = t_ref[:, c * chunk : (c + 1) * chunk]
        right = t_ref[:, half + c * chunk : half + (c + 1) * chunk]
        for j, folded in enumerate((left + right, left - right)):
            lanes = slice(j * band, (j + 1) * band)
            table = (tab["column"][0, :, lanes], tab["column"][1, :, lanes])
            got = dot3(split(folded), table)
            cosine, sine = got[:, : band // 2], got[:, band // 2 :]
            near = slice(j * band // 2, (j + 1) * band // 2)
            far = slice(band + j * band // 2, band + (j + 1) * band // 2)
            if c == 0:
                acc[:, near] = cosine
                acc[:, far] = sine
            else:
                tc = tab["twiddle"][c, 0:1, near]
                ts = tab["twiddle"][c, 1:2, near]
                acc[:, near] += cosine * tc - sine * ts
                acc[:, far] += sine * tc + cosine * ts

    k_load.start()
    for name in ("sample", "window", "spread"):
        loads[name].start()
    loads["order"].wait()
    loads["row"].wait()
    loads["phase"].wait()
    ordered = [
        [dot(p, tab["order"][...]) for p in split(acc[:, lanes])]
        for lanes in (slice(0, band), slice(band, 2 * band))
    ]
    columns = [
        jnp.concatenate([ordered[0][i].astype(jnp.bfloat16), ordered[1][i].astype(jnp.bfloat16)], axis=1)
        for i in range(2)
    ]
    z = dot3((tab["row"][0], tab["row"][1]), columns)
    zcc, zcs, zsc, zss = z[:low, :band], z[:low, band:], z[low:, :band], z[low:, band:]
    lane = lax.broadcasted_iota(jnp.int32, tab["phase"].shape[1:], 1)
    pc = jnp.sum(jnp.where(lane == me, tab["phase"][0], 0.0), axis=1, keepdims=True)
    ps = jnp.sum(jnp.where(lane == me, tab["phase"][1], 0.0), axis=1, keepdims=True)
    nc, ns = pc[:low], ps[:low]
    re, im = zcc - zss, -(zcs + zsc)
    re, im = re * nc + im * ns, im * nc - re * ns
    sbuf[:low, :] = re[:, :low]
    sbuf[low : 2 * low, :] = re[:, low:]
    sbuf[2 * low : 3 * low, :] = im[:, :low]
    sbuf[3 * low :, :] = im[:, low:]
    esend[0:1, :band] = jnp.sum(ordered[0][0] + ordered[0][1], axis=0, keepdims=True)
    esend[0:1, band : 2 * band] = -jnp.sum(ordered[1][0] + ordered[1][1], axis=0, keepdims=True)
    re, im = (zcc + zss)[:, :low], (zcs - zsc)[:, :low]
    re, im = re * nc + im * ns, im * nc - re * ns
    esend[0:1, 2 * band : 2 * band + low] = re.T[0:1]
    esend[0:1, 2 * band + low :] = im.T[0:1]

    pl.semaphore_wait(barrier, chips)
    length = chips * part
    mine = pl.ds(pl.multiple_of(core * length, length), length)
    theirs = pl.ds(pl.multiple_of((1 - core) * length, length), length)
    pair = remote(sbuf.at[theirs], pbuf, 0, 0, partner)
    epair = remote(esend, erecv.at[0], 1, 0, partner)
    pair.start()
    epair.start()
    pair.wait_recv()
    csum[...] = sbuf[mine, :] + pbuf[...]
    epair.wait_recv()
    epsum[...] = esend[...] + erecv[0]
    sends, esends = [], []
    for k in range(1, chips):
        to = lax.rem(chip + k, chips)
        piece = pl.ds(pl.multiple_of(to * part, part), part)
        sends.append(remote(csum.at[piece], rbuf.at[k - 1], 0, k, peer(k)))
        esends.append(remote(epsum, erecv.at[k], 1, k, peer(k)))
        sends[-1].start()
        esends[-1].start()
    total = csum[pl.ds(pl.multiple_of(chip * part, part), part), :]
    for k in range(1, chips):
        sends[k - 1].wait_recv()
        total = total + rbuf[k - 1]
    own = place(chip, core)
    fbuf[own, :] = total
    shares = [remote(fbuf.at[own], fbuf.at[own], 2, k, peer(k)) for k in range(1, chips)]
    for share in shares:
        share.start()
    passed = [remote(fbuf.at[own], fbuf.at[own], 3, 0, partner)]
    passed[0].start()
    edge = epsum[...]
    for k in range(1, chips):
        esends[k - 1].wait_recv()
        edge = edge + erecv[k]
    k_load.wait()
    for name in ("sample", "window", "spread"):
        loads[name].wait()
    for k in range(1, chips):
        shares[k - 1].wait_recv()
        region = fbuf.at[place(lax.rem(chip - k + chips, chips), core)]
        passed.append(remote(region, region, 3, k, partner))
        passed[-1].start()
    for p in passed:
        p.wait_recv()

    mre = jnp.concatenate([fbuf[:low, :], fbuf[low : 2 * low, :]], axis=1)
    mim = jnp.concatenate([fbuf[2 * low : 3 * low, :], fbuf[3 * low :, :]], axis=1)
    cells = [lax.broadcasted_iota(jnp.int32, (band, band), i) for i in range(2)]
    mirror = (cells[0] + cells[1] == band).astype(jnp.float32).astype(jnp.bfloat16)
    cells = [lax.broadcasted_iota(jnp.int32, (low, low), i) for i in range(2)]
    flip = (cells[0] + cells[1] == low).astype(jnp.float32).astype(jnp.bfloat16)
    turned = dot(jnp.concatenate([*split(mre), *split(mim)], axis=0), mirror)
    first = lax.broadcasted_iota(jnp.int32, (low, band), 1) == 0
    parts = []
    for i in range(2):
        both = turned[2 * i * low : (2 * i + 1) * low] + turned[(2 * i + 1) * low : (2 * i + 2) * low]
        corner = edge[:, 2 * band + i * low : 2 * band + (i + 1) * low]
        corner = jnp.broadcast_to(corner, (low, low)).T[:, 0:1]
        parts += split(jnp.where(first, corner, both))
    flipped = dot(flip, jnp.concatenate(parts, axis=1))
    top = lax.broadcasted_iota(jnp.int32, (low, band), 0) == 0
    fre = jnp.where(top, edge[:, :band], flipped[:, :band] + flipped[:, band : 2 * band])
    fim = jnp.where(top, edge[:, band : 2 * band], -(flipped[:, 2 * band : 3 * band] + flipped[:, 3 * band :]))

    norm = 1.0 / (side * band)
    re = jnp.concatenate([mre, fre], axis=0)
    im = jnp.concatenate([mim, fim], axis=0)
    spec[:band, :] = (re * pc - im * ps) * norm
    spec[band:, :] = (im * pc + re * ps) * norm

    def one(k, carry):
        sr, si = spec[:band, :], spec[band:, :]
        kr, ki = k_ref[k, 0], k_ref[k, 1]
        rh, rl = split(kr * sr - ki * si)
        ih, il = split(kr * si + ki * sr)
        high = jnp.concatenate([rh, ih], axis=0)
        low = jnp.concatenate([rl, il], axis=0)
        wide = dot(tab["sample"][...], high)
        lbuf[k] = wide[: 2 * samples] + wide[2 * samples :] + dot(tab["sample"][: 2 * samples, :], low)
        return carry

    lax.fori_loop(0, kernels, one, 0, unroll=True)
    left = split(lbuf[...].reshape(kernels * 2 * samples, band))
    field = dot3(left, (tab["window"][0], tab["window"][1]))
    width = field.shape[1] // 2
    field = field.reshape(kernels, 2 * samples, 2 * width)
    fr = field[:, :samples, :width] - field[:, samples:, width:]
    fi = field[:, :samples, width:] + field[:, samples:, :width]
    intensity = jnp.sum(fr * fr + fi * fi, axis=0) * (1.0 / kernels)
    blurred = binomial[0] * intensity
    for v in range(1, 5):
        blurred = blurred + binomial[v] * pltpu.roll(intensity, width - v, 1)
    ibuf[0] = blurred[:, :COLS]

    rings = [
        remote(ibuf.at[0], ibuf.at[slabs - 2 * k], 4, k, peer(k)) for k in range(1, chips)
    ]
    for ring in rings:
        ring.start()
    beside = [remote(ibuf.at[0], ibuf.at[lax.rem(slabs - 1 + 2 * core, slabs)], 5, 0, partner)]
    beside[0].start()
    for k in range(1, chips):
        rings[k - 1].wait_recv()
        slot = lax.rem(slabs - 2 * k - 1 + 2 * core + slabs, slabs)
        beside.append(remote(ibuf.at[slabs - 2 * k], ibuf.at[slot], 5, k, partner))
        beside[-1].start()
    for b in beside:
        b.wait_recv()
    gathered = split(ibuf[...].reshape(slabs * samples, COLS))
    out[...] = dot3((tab["spread"][0], tab["spread"][1]), gathered)
    for copy in [pair, epair] + sends + esends + shares + passed + rings + beside:
        copy.wait_send()


def local(transmission, kernel_spectra):
    slabs = lax.axis_size("slab")
    rows, side = transmission.shape
    kernels, _, band, _ = kernel_spectra.shape
    chunk = min(CHUNK, side // 2)
    consts = tables(slabs, rows, side, band, chunk)
    arrays = [jnp.asarray(consts[name]) for name in NAMES]
    samples = rows * 2 * band // side
    part = 2 * band // slabs
    chips, low = slabs // 2, band // 2
    any_spec = pl.BlockSpec(memory_space=pl.ANY)
    return pl.pallas_call(
        functools.partial(body, slabs, chunk),
        out_shape=jax.ShapeDtypeStruct((rows, COLS), jnp.float32),
        in_specs=[any_spec] * (2 + len(NAMES)),
        out_specs=pl.BlockSpec(memory_space=pltpu.VMEM),
        scratch_shapes=[
            pltpu.VMEM(transmission.shape, jnp.float32),
            pltpu.VMEM(kernel_spectra.shape, jnp.float32),
            *[pltpu.VMEM(a.shape, a.dtype) for a in arrays],
            pltpu.VMEM((rows, 2 * band), jnp.float32),
            pltpu.VMEM((2 * band, low), jnp.float32),
            pltpu.VMEM((chips * part, low), jnp.float32),
            pltpu.VMEM((chips * part, low), jnp.float32),
            pltpu.VMEM((chips - 1, part, low), jnp.float32),
            pltpu.VMEM((2 * band, low), jnp.float32),
            pltpu.VMEM((1, 3 * band), jnp.float32),
            pltpu.VMEM((1, 3 * band), jnp.float32),
            pltpu.VMEM((chips, 1, 3 * band), jnp.float32),
            pltpu.VMEM((2 * band, band), jnp.float32),
            pltpu.VMEM((kernels, 2 * samples, band), jnp.float32),
            pltpu.VMEM((slabs, samples, COLS), jnp.float32),
            pltpu.SemaphoreType.DMA((len(NAMES) + 1,)),
            pltpu.SemaphoreType.DMA((2 * (side // 2 // chunk),)),
            pltpu.SemaphoreType.DMA((6, chips)),
            pltpu.SemaphoreType.DMA((6, chips)),
        ],
        compiler_params=pltpu.CompilerParams(
            collective_id=0, has_side_effects=True, vmem_limit_bytes=67_043_328
        ),
    )(transmission, kernel_spectra, *arrays)


def solution(mesh):
    return jax.shard_map(
        local,
        mesh=mesh,
        in_specs=(P(("tiles", "slab"), None), P()),
        out_specs=P(("tiles", "slab"), None),
        check_vma=False,
    )
```
